32 devices in a mesh: gx: 2 (over core), gy: 16 (over z, y, x).
Axes of the slice: x: 2, y: 2, z: 4, core: 2. Of those that a mesh axis runs over, the one named last changes fastest.
Arguments:
- right_side: float32 [128, 4096], P('gx', 'gy'), may hold values from -34 to 34, as said below
- initial: float32 [128, 4096], P('gx', 'gy'), may hold values from -0.6 to 0.6
- reaction: float32 [128, 4096], P('gx', 'gy'), may hold values from 0.05 to 0.5
- velocity_x: float32 [128, 4096], P('gx', 'gy'), may hold values from -1 to 1
- velocity_y: float32 [128, 4096], P('gx', 'gy'), may hold values from -1 to 1
Outputs:
- solution: float32 [128, 4096], P('gx', 'gy')
- residual: float32 [128, 4096], P('gx', 'gy')
The draws below stay inside these ranges and needn't reach their ends.
Inputs may be any that keep to these rules, and one draw needn't show every extreme that they name: right_side is noise bounded by 4 in size times an envelope 0.5 + 8 g, where g is a periodic Gaussian bump of one device block's width along each dimension centred at a drawn position, so its entries lie within -34 and 34.
All inputs are finite; a program needn't handle non-finite values.
Results may differ from the reference program's by a relative error of at most 0.0075.
Values sent between devices are 32-bit elements.
A program may use at most 64 MiB of HBM per device.

```python
import math
import jax
import jax.numpy as jnp
from jax import lax

CX = 64
CY = 256
RESTART = 15
NX = 128
NY = 4096


def draw_right_side(key, part):
    noise_key = jax.random.fold_in(key, 11)
    centre_key = jax.random.fold_in(key, 12)
    noise = jnp.clip(jax.random.normal(noise_key, (NX, NY), jnp.float32), -4.0, 4.0)
    centre = jax.random.uniform(centre_key, (2,), jnp.float32)
    along_x = jnp.mod(jnp.arange(NX, dtype=jnp.float32) - centre[0] * NX, NX)
    along_y = jnp.mod(jnp.arange(NY, dtype=jnp.float32) - centre[1] * NY, NY)
    gap_x = jnp.minimum(along_x, NX - along_x) / CX
    gap_y = jnp.minimum(along_y, NY - along_y) / CY
    bump = jnp.exp(-0.5 * (gap_x[:, None] * gap_x[:, None] + gap_y[None, :] * gap_y[None, :]))
    return noise * (0.5 + 8.0 * bump)


def block_levels(key, dims, pieces, smallest, top_value):
    def one(dim, parts):
        draws = jax.random.uniform(jax.random.fold_in(jax.random.fold_in(key, 6), dim), (parts,), jnp.float32, smallest / len(pieces), top_value / len(pieces))
        return jnp.repeat(jnp.exp(draws), dims[dim] // parts).reshape((-1,) + (1,) * (len(dims) - dim - 1))

    gain = one(*pieces[0])
    for cut in pieces[1:]:
        gain = gain * one(*cut)
    return gain


def scatter_about(stream_key, extent, deviation, limit, split=(), held_as=jnp.bfloat16):
    loudness = block_levels(stream_key, extent, split, -0.22, 0.18) if split else 1.0
    drawn = jax.random.normal(stream_key, extent, jnp.float32) * deviation * loudness
    return jnp.minimum(jnp.maximum(drawn, -limit), limit).astype(held_as)


def setup_inputs(seed: int = 0) -> dict:
    arg_keys = jax.random.split(jax.random.key(seed), 6)
    return {
        "right_side": draw_right_side(jax.random.fold_in(arg_keys[5], 71), 0),
        "initial": scatter_about(arg_keys[1], (NX, NY), 0.1, 0.6, ((0, 2), (1, 16)), jnp.float32),
        "reaction": jnp.clip(jnp.exp(math.log(0.5) - 2.3025851 * jax.random.uniform(arg_keys[2], (NX, NY), jnp.float32) ** block_levels(arg_keys[2], (NX, NY), ((0, 2), (1, 16)), -0.2, 0.2)), 0.05, 0.5),
        "velocity_x": jnp.clip(jax.random.uniform(arg_keys[3], (NX, NY), jnp.float32, -1.0, 1.0) * block_levels(arg_keys[3], (NX, NY), ((0, 2), (1, 16)), -0.4, 0.0), -1.0, 1.0),
        "velocity_y": jnp.clip(jax.random.uniform(arg_keys[4], (NX, NY), jnp.float32, -1.0, 1.0) * block_levels(arg_keys[4], (NX, NY), ((0, 2), (1, 16)), -0.4, 0.0), -1.0, 1.0),
    }


def moved(field, offset, dimension):
    return jnp.roll(field, -offset, dimension)

def first_diff(field, dimension):
    outer = moved(field, -2, dimension) - moved(field, 2, dimension)
    inner = moved(field, 1, dimension) - moved(field, -1, dimension)
    return (outer + 8.0 * inner) / 12.0

def second_diff(field, dimension):
    inner = moved(field, 1, dimension) + moved(field, -1, dimension)
    outer = moved(field, 2, dimension) + moved(field, -2, dimension)
    return (16.0 * inner - outer - 30.0 * field) / 12.0

def operate(field, reaction, velocity_x, velocity_y):
    diffusion = second_diff(field, 0) + second_diff(field, 1)
    advect_x = 0.5 * (velocity_x * first_diff(field, 0) + first_diff(velocity_x * field, 0))
    advect_y = 0.5 * (velocity_y * first_diff(field, 1) + first_diff(velocity_y * field, 1))
    return reaction * field - diffusion + advect_x + advect_y

def least_squares(hessenberg, beta):
    columns_total = hessenberg.shape[1]
    target = jnp.where(jnp.arange(columns_total + 1) == 0, beta, 0.0)

    def rotate(column, carried):
        upper, target = carried
        top_row = upper[column]
        next_row = upper[column + 1]
        diagonal_entry = top_row[column]
        below_entry = next_row[column]
        radius = jnp.sqrt(diagonal_entry * diagonal_entry + below_entry * below_entry)
        cosine = diagonal_entry / radius
        sine_value = below_entry / radius
        upper = upper.at[column].set(cosine * top_row + sine_value * next_row)
        upper = upper.at[column + 1].set(cosine * next_row - sine_value * top_row)
        upper_value = target[column]
        lower_value = target[column + 1]
        target = target.at[column].set(cosine * upper_value + sine_value * lower_value)
        target = target.at[column + 1].set(cosine * lower_value - sine_value * upper_value)
        return (upper, target)
    upper, target = lax.fori_loop(0, columns_total, rotate, (hessenberg, target))

    def substitute(count, weights):
        row_index = columns_total - 1 - count
        known = jnp.sum(upper[row_index] * weights)
        return weights.at[row_index].set((target[row_index] - known) / upper[row_index, row_index])
    return lax.fori_loop(0, columns_total, substitute, jnp.zeros((columns_total,), jnp.float32))

def reference(right_side, initial, reaction, velocity_x, velocity_y):

    def operator_on(field):
        return operate(field, reaction, velocity_x, velocity_y)
    start_residual = right_side - operator_on(initial)
    beta = jnp.sqrt(jnp.sum(start_residual * start_residual))
    basis = [start_residual / beta]
    hessenberg = jnp.zeros((RESTART + 1, RESTART), jnp.float32)
    for column in range(RESTART):
        applied = operator_on(basis[column])
        projection = jnp.stack([jnp.sum(vector * applied) for vector in basis])
        correction = jnp.zeros_like(applied)
        for position, vector in enumerate(basis):
            correction = correction + projection[position] * vector
        applied = applied - correction
        length = jnp.sqrt(jnp.sum(applied * applied))
        hessenberg = hessenberg.at[:column + 1, column].set(projection)
        hessenberg = hessenberg.at[column + 1, column].set(length)
        basis.append(applied / length)
    weights = least_squares(hessenberg, beta)
    solution = initial
    for position in range(RESTART):
        solution = solution + weights[position] * basis[position]
    residual = right_side - operator_on(solution)
    return (solution, residual)
```

```python
import functools

import jax
import jax.numpy as jnp
from jax import lax
from jax.experimental import pallas as pl
from jax.experimental.pallas import tpu as pltpu
from jax.sharding import PartitionSpec as P

RESTART = 15
HALO = 2 * (RESTART + 1)
LANES = 128
PAD = 8
CENTRE = 5.5
HALF_WIDTH = 5.2
REFINEMENTS = 3
MESH = pl.DeviceIdType.MESH


def two_sum(a, b):
    total = a + b
    shown = total - a
    return total, (a - (total - shown)) + (b - shown)


def add_pairs(a, b):
    total, rest = two_sum(a[0], b[0])
    return total, rest + (a[1] + b[1])


def split(a):
    scaled = a * 4097.0
    high = scaled - (scaled - a)
    return high, a - high


def two_product(a, b):
    product = a * b
    ah, al = split(a)
    bh, bl = split(b)
    return product, ((ah * bh - product) + ah * bl + al * bh) + al * bl


def tree(items, combine):
    items = list(items)
    while len(items) > 1:
        paired = [combine(items[i], items[i + 1]) for i in range(0, len(items) - 1, 2)]
        items = paired + (items[-1:] if len(items) % 2 else [])
    return items[0]


def rolled(x, shift, axis):
    shift %= x.shape[axis]
    return x if shift == 0 else pltpu.roll(x, shift, axis)


def kernel(
    nx_dev, ny_dev,
    b_ref, x0_ref, re_ref, vx_ref, vy_ref, sol_ref, res_ref,
    pack_r, pack_l, from_l, from_r, other, field, coef, centre, vec, app, acc, gram,
    out_sem, in_sem, gram_out, gram_in,
):
    rows, cols = b_ref.shape
    own_tiles = cols // LANES
    tiles = own_tiles + 1
    all_rows = nx_dev * rows
    n_dev = nx_dev * ny_dev
    gx, gy = lax.axis_index("gx"), lax.axis_index("gy")
    me = gx * ny_dev + gy
    partner = 1 - gx
    right, left = lax.rem(gy + 1, ny_dev), lax.rem(gy + ny_dev - 1, ny_dev)
    inputs = (x0_ref, vx_ref, vy_ref, re_ref, b_ref)
    fold = rows // 4

    def device(step):
        target = lax.rem(me + step, n_dev)
        return target // ny_dev, lax.rem(target, ny_dev)

    barrier = pltpu.get_barrier_semaphore()

    def greet(step, carry):
        pl.semaphore_signal(barrier, inc=1, device_id=device(step), device_id_type=MESH)
        return carry

    lax.fori_loop(1, n_dev, greet, 0)

    lane = lax.broadcasted_iota(jnp.int32, (8, LANES), 1)
    lane_f = lax.broadcasted_iota(jnp.int32, (fold, LANES), 1)

    for pack, tile, base in ((pack_r, own_tiles - 1, LANES - HALO), (pack_l, 0, 0)):
        at = slice(tile * LANES, (tile + 1) * LANES)
        for r in range(0, rows, fold):
            parts = [
                rolled(inputs[f][r:r + fold, at], 32 * f - base, 1) for f in range(4)
            ]
            packed = parts[3]
            for f in (2, 1, 0):
                packed = jnp.where(lane_f < 32 * (f + 1), parts[f], packed)
            pack[r:r + fold, :] = packed
        parts = [rolled(b_ref[q * fold:(q + 1) * fold, at], 32 * q - base, 1) for q in range(4)]
        packed = parts[3]
        for q in (2, 1, 0):
            packed = jnp.where(lane_f < 32 * (q + 1), parts[q], packed)
        pack[rows:rows + fold, :] = packed

    pl.semaphore_wait(barrier, n_dev - 1)

    copies = []

    def send(src, dst, target):
        k = len(copies)
        copy = pltpu.make_async_remote_copy(
            src_ref=src, dst_ref=dst, send_sem=out_sem.at[k], recv_sem=in_sem.at[k],
            device_id=target, device_id_type=MESH,
        )
        copy.start()
        copies.append(copy)

    send(pack_r, from_l.at[0], (gx, right))
    send(pack_l, from_r.at[0], (gx, left))
    send(pack_r, from_l.at[1], (partner, right))
    send(pack_l, from_r.at[1], (partner, left))
    for f in range(5):
        send(inputs[f], other.at[f], (partner, gy))

    for f in range(5):
        for t in range(own_tiles):
            field[f, t, PAD:PAD + rows, :] = inputs[f][:, t * LANES:(t + 1) * LANES]
    for f in range(5):
        copies[4 + f].wait()
        for t in range(own_tiles):
            field[f, t, PAD + rows:PAD + all_rows, :] = other[f, :, t * LANES:(t + 1) * LANES]
    for k in range(4):
        copies[k].wait()
    for h in range(2):
        for f in range(5):
            for r in range(0, rows, fold):
                if f < 4:
                    off = 32 * f
                    at_r, at_l = from_r[h, r:r + fold, :], from_l[h, r:r + fold, :]
                else:
                    off = 32 * (r // fold)
                    at_r, at_l = from_r[h, rows:rows + fold, :], from_l[h, rows:rows + fold, :]
                edge = jnp.where(
                    lane_f < HALO, rolled(at_r, -off, 1),
                    jnp.where(lane_f >= LANES - HALO, rolled(at_l, LANES - HALO - off, 1), 0.0),
                )
                start = PAD + h * rows + r
                field[f, own_tiles, start:start + fold, :] = edge

    def wrap(ref, t):
        ref[t, 0:PAD, :] = ref[t, all_rows:all_rows + PAD, :]
        ref[t, PAD + all_rows:2 * PAD + all_rows, :] = ref[t, PAD:2 * PAD, :]

    for f in range(2):
        for t in range(tiles):
            wrap(field.at[f], t)

    chunk = 16
    lane_c = lax.broadcasted_iota(jnp.int32, (chunk, LANES), 1)

    def along(values, offset):
        shifted = [rolled(v, -offset, 1) for v in values]
        step = 1 if offset > 0 else -1
        keep = lane_c < LANES - offset if offset > 0 else lane_c >= -offset
        return [
            jnp.where(keep, shifted[t], shifted[(t + step) % tiles]) for t in range(tiles)
        ]

    offsets = (-2, -1, 1, 2)
    plain = {-2: 1.0 / 12.0, -1: -4.0 / 3.0, 1: -4.0 / 3.0, 2: 1.0 / 12.0}
    speed = {-2: 1.0 / 24.0, -1: -1.0 / 3.0, 1: 1.0 / 3.0, 2: -1.0 / 24.0}

    for r in range(0, all_rows, chunk):
        here = slice(PAD + r, PAD + r + chunk)
        vy = [field[2, t, here, :] for t in range(tiles)]
        for n, o in enumerate(offsets):
            moved = along(vy, o)
            for t in range(tiles):
                vx = field[1, t, here, :]
                vx_o = field[1, t, PAD + r + o:PAD + r + o + chunk, :]
                coef[n, t, r:r + chunk, :] = plain[o] + speed[o] * (vx + vx_o)
                coef[4 + n, t, r:r + chunk, :] = plain[o] + speed[o] * (vy[t] + moved[t])
        for t in range(tiles):
            centre[t, r:r + chunk, :] = 5.0 + field[3, t, here, :]

    def operate(src, r):
        here = slice(PAD + r, PAD + r + chunk)
        u = [src[t, here, :] for t in range(tiles)]
        total = [centre[t, r:r + chunk, :] * u[t] for t in range(tiles)]
        for n, o in enumerate(offsets):
            moved = along(u, o)
            for t in range(tiles):
                u_o = src[t, PAD + r + o:PAD + r + o + chunk, :]
                total[t] = total[t] + (
                    coef[n, t, r:r + chunk, :] * u_o + coef[4 + n, t, r:r + chunk, :] * moved[t]
                )
        return u, total

    x0 = field.at[0]
    for r in range(0, all_rows, chunk):
        here = slice(PAD + r, PAD + r + chunk)
        _, total = operate(x0, r)
        for t in range(tiles):
            r0 = field[4, t, here, :] - total[t]
            vec[1, t, here, :] = r0
            vec[0, t, here, :] = jnp.zeros_like(r0)
            if r < rows and t < own_tiles:
                app[RESTART, t, r:r + chunk, :] = r0
    for t in range(tiles):
        wrap(vec.at[1], t)

    def step(k, carry):
        src = vec.at[k + 1]
        a = jnp.where(k == 0, 1.0 / HALF_WIDTH, 2.0 / HALF_WIDTH).astype(jnp.float32)
        for r in range(0, all_rows, chunk):
            here = slice(PAD + r, PAD + r + chunk)
            u, total = operate(src, r)
            for t in range(tiles):
                if r < rows and t < own_tiles:
                    app[k, t, r:r + chunk, :] = total[t]
                vec[k + 2, t, here, :] = a * (total[t] - CENTRE * u[t]) - vec[k, t, here, :]
        for t in range(tiles):
            wrap(vec.at[k + 2], t)
        return carry

    lax.fori_loop(0, RESTART, step, 0)

    size = RESTART + 1
    places = [(t, r) for t in range(own_tiles) for r in range(0, rows, 8)]
    for i in range(size):
        mine = [app[i, t, r:r + 8, :] for t, r in places]
        for j in range(i + 1):
            if j == i:
                value = tree([m * m for m in mine], lambda a, b: a + b)
            else:
                value = tree(
                    [m * app[j, t, r:r + 8, :] for m, (t, r) in zip(mine, places)],
                    lambda a, b: a + b,
                )
            for p, q in {(i, j), (j, i)}:
                at = (p * size + q) * 8
                acc[at:at + 8, :] = value

    packed = jnp.zeros((8, LANES), jnp.float32)
    for i in range(size):
        for h in range(2):
            base = (i * size + 8 * h) * 8
            pair = tree(
                [
                    (acc[pl.ds(base + s, 8, stride=8), :], jnp.zeros((8, LANES), jnp.float32))
                    for s in range(8)
                ],
                add_pairs,
            )
            shift = LANES // 2
            while shift:
                pair = add_pairs(pair, tuple(rolled(p, shift, 1) for p in pair))
                shift //= 2
            packed = jnp.where(lane == 32 * h + i, pair[0], packed)
            packed = jnp.where(lane == 32 * h + 16 + i, pair[1], packed)
    gram[me] = packed

    def gram_copy(slot, target):
        return pltpu.make_async_remote_copy(
            src_ref=gram.at[me], dst_ref=gram.at[me], send_sem=gram_out.at[slot],
            recv_sem=gram_in.at[me], device_id=target, device_id_type=MESH,
        )

    def gram_send(step, carry):
        gram_copy(step, device(step)).start()
        return carry

    lax.fori_loop(1, n_dev, gram_send, 0)

    def gram_wait(step, carry):
        source = lax.rem(me + step, n_dev)
        pltpu.make_async_remote_copy(
            src_ref=gram.at[me], dst_ref=gram.at[source], send_sem=gram_out.at[step],
            recv_sem=gram_in.at[source], device_id=device(step), device_id_type=MESH,
        ).wait()
        return carry

    lax.fori_loop(1, n_dev, gram_wait, 0)

    def as_pair(value):
        return (
            jnp.where(lane % 32 < 16, value, 0.0),
            jnp.where(lane % 32 < 16, rolled(value, -16, 1), 0.0),
        )

    total = tree([as_pair(gram[d]) for d in range(n_dev)], add_pairs)

    def unpack(value):
        low = jnp.where(lane < 16, value, 0.0)
        high = jnp.where(lane < 16, rolled(value, -32, 1), 0.0)
        return jnp.concatenate([low, high], axis=0)

    g_high, g_low = unpack(total[0]), unpack(total[1])
    row_g = lax.broadcasted_iota(jnp.int32, (size, LANES), 0)
    lane_g = lax.broadcasted_iota(jnp.int32, (size, LANES), 1)
    m = g_high + jnp.where(lane_g - 16 == row_g, 1.0, 0.0)
    for k in range(RESTART):
        pivot = m[k:k + 1, :] / m[k:k + 1, k:k + 1]
        m = jnp.where(row_g == k, pivot, m - m[:, k:k + 1] * pivot)
    z = jnp.where(row_g < RESTART, jnp.broadcast_to(m[:, RESTART:size], m.shape), -1.0)
    inverse = jnp.where((lane_g < RESTART) & (row_g < RESTART), rolled(m, -16, 1), 0.0)
    for _ in range(REFINEMENTS):
        high, low = two_product(g_high, z)
        low = low + g_low * z
        pair = add_pairs((high[0:8], low[0:8]), (high[8:16], low[8:16]))
        for shift in (4, 2, 1):
            pair = add_pairs(pair, tuple(rolled(p, shift, 0) for p in pair))
        rest = pair[0] + pair[1]
        change = inverse * jnp.concatenate([rest, rest], axis=0)
        z = z - jnp.sum(change, axis=1, keepdims=True)

    weights = [jnp.broadcast_to(z[k:k + 1, :], (8, LANES)) for k in range(RESTART)]
    for t, r in places:
        at = slice(t * LANES, (t + 1) * LANES)
        up = tree(
            [weights[k] * vec[1 + k, t, PAD + r:PAD + r + 8, :] for k in range(RESTART)],
            lambda a, b: a + b,
        )
        sol_ref[r:r + 8, at] = x0_ref[r:r + 8, at] + up
        down = tree(
            [weights[k] * app[k, t, r:r + 8, :] for k in range(RESTART)], lambda a, b: a + b
        )
        res_ref[r:r + 8, at] = app[RESTART, t, r:r + 8, :] - down


def shards(nx_dev, ny_dev, right_side, initial, reaction, velocity_x, velocity_y):
    rows, cols = right_side.shape
    tiles = cols // LANES + 1
    all_rows = nx_dev * rows
    n_dev = nx_dev * ny_dev
    size = RESTART + 1
    padded = all_rows + 2 * PAD
    pack = (rows + rows // 4, LANES)
    f32 = jnp.float32
    out = jax.ShapeDtypeStruct((rows, cols), f32)
    vmem = pl.BlockSpec(memory_space=pltpu.VMEM)
    return pl.pallas_call(
        functools.partial(kernel, nx_dev, ny_dev),
        out_shape=(out, out),
        in_specs=[vmem] * 5,
        out_specs=(vmem, vmem),
        scratch_shapes=[
            pltpu.VMEM(pack, f32),
            pltpu.VMEM(pack, f32),
            pltpu.VMEM((2,) + pack, f32),
            pltpu.VMEM((2,) + pack, f32),
            pltpu.VMEM((5, rows, cols), f32),
            pltpu.VMEM((5, tiles, padded, LANES), f32),
            pltpu.VMEM((8, tiles, all_rows, LANES), f32),
            pltpu.VMEM((tiles, all_rows, LANES), f32),
            pltpu.VMEM((RESTART + 2, tiles, padded, LANES), f32),
            pltpu.VMEM((size, cols // LANES, rows, LANES), f32),
            pltpu.VMEM((size * size * 8, LANES), f32),
            pltpu.VMEM((n_dev, 8, LANES), f32),
            pltpu.SemaphoreType.DMA((9,)),
            pltpu.SemaphoreType.DMA((9,)),
            pltpu.SemaphoreType.DMA((n_dev,)),
            pltpu.SemaphoreType.DMA((n_dev,)),
        ],
        compiler_params=pltpu.CompilerParams(collective_id=0, has_side_effects=True),
        name="gmres_cycle",
    )(right_side, initial, reaction, velocity_x, velocity_y)


def solution(mesh):
    spec = P("gx", "gy")
    return jax.shard_map(
        functools.partial(shards, mesh.shape["gx"], mesh.shape["gy"]),
        mesh=mesh,
        in_specs=(spec,) * 5,
        out_specs=(spec, spec),
        check_vma=False,
    )
```

```python
import functools

import jax
import jax.numpy as jnp
from jax import lax
from jax.experimental import pallas as pl
from jax.experimental.pallas import tpu as pltpu
from jax.sharding import PartitionSpec as P

RESTART = 15
HALO = 2 * (RESTART + 1)
LANES = 128
PAD = 8
CENTRE = 5.5
HALF_WIDTH = 5.2
REFINEMENTS = 2
MESH = pl.DeviceIdType.MESH


def two_sum(a, b):
    total = a + b
    shown = total - a
    return total, (a - (total - shown)) + (b - shown)


def add_pairs(a, b):
    total, rest = two_sum(a[0], b[0])
    return total, rest + (a[1] + b[1])


def split(a):
    scaled = a * 4097.0
    high = scaled - (scaled - a)
    return high, a - high


def two_product(a, b):
    product = a * b
    ah, al = split(a)
    bh, bl = split(b)
    return product, ((ah * bh - product) + ah * bl + al * bh) + al * bl


def tree(items, combine):
    items = list(items)
    while len(items) > 1:
        paired = [combine(items[i], items[i + 1]) for i in range(0, len(items) - 1, 2)]
        items = paired + (items[-1:] if len(items) % 2 else [])
    return items[0]


def rolled(x, shift, axis):
    shift %= x.shape[axis]
    return x if shift == 0 else pltpu.roll(x, shift, axis)


def kernel(
    nx_dev, ny_dev,
    b_ref, x0_ref, re_ref, vx_ref, vy_ref, sol_ref, res_ref,
    pack_r, pack_l, from_l, from_r, other, field, coef, centre, vec, app, acc, gram,
    out_sem, in_sem, gram_out, gram_in,
):
    rows, cols = b_ref.shape
    own_tiles = cols // LANES
    tiles = own_tiles + 1
    all_rows = nx_dev * rows
    n_dev = nx_dev * ny_dev
    gx, gy = lax.axis_index("gx"), lax.axis_index("gy")
    me = gx * ny_dev + gy
    partner = 1 - gx
    right, left = lax.rem(gy + 1, ny_dev), lax.rem(gy + ny_dev - 1, ny_dev)
    inputs = (x0_ref, vx_ref, vy_ref, re_ref, b_ref)
    fold = rows // 4

    barrier = pltpu.get_barrier_semaphore()

    def greet(step, carry):
        there = lax.rem(gy + step, ny_dev)
        for core in (gx, partner):
            pl.semaphore_signal(barrier, inc=1, device_id=(core, there), device_id_type=MESH)
        return carry

    pl.semaphore_signal(barrier, inc=1, device_id=(partner, gy), device_id_type=MESH)
    lax.fori_loop(1, ny_dev, greet, 0)

    lane = lax.broadcasted_iota(jnp.int32, (8, LANES), 1)
    lane_f = lax.broadcasted_iota(jnp.int32, (fold, LANES), 1)

    for pack, tile, base in ((pack_r, own_tiles - 1, LANES - HALO), (pack_l, 0, 0)):
        at = slice(tile * LANES, (tile + 1) * LANES)
        for r in range(0, rows, fold):
            parts = [
                rolled(inputs[f][r:r + fold, at], 32 * f - base, 1) for f in range(4)
            ]
            packed = parts[3]
            for f in (2, 1, 0):
                packed = jnp.where(lane_f < 32 * (f + 1), parts[f], packed)
            pack[r:r + fold, :] = packed
        parts = [rolled(b_ref[q * fold:(q + 1) * fold, at], 32 * q - base, 1) for q in range(4)]
        packed = parts[3]
        for q in (2, 1, 0):
            packed = jnp.where(lane_f < 32 * (q + 1), parts[q], packed)
        pack[rows:rows + fold, :] = packed

    for f in range(5):
        for t in range(own_tiles):
            field[f, t, PAD:PAD + rows, :] = inputs[f][:, t * LANES:(t + 1) * LANES]

    pl.semaphore_wait(barrier, n_dev - 1)

    copies = []

    def send(src, dst, target):
        k = len(copies)
        copy = pltpu.make_async_remote_copy(
            src_ref=src, dst_ref=dst, send_sem=out_sem.at[k], recv_sem=in_sem.at[k],
            device_id=target, device_id_type=MESH,
        )
        copy.start()
        copies.append(copy)

    send(pack_r, from_l.at[0], (gx, right))
    send(pack_l, from_r.at[0], (gx, left))
    send(pack_r, from_l.at[1], (partner, right))
    send(pack_l, from_r.at[1], (partner, left))
    for f in range(5):
        send(inputs[f], other.at[f], (partner, gy))

    for f in range(5):
        copies[4 + f].wait()
        for t in range(own_tiles):
            field[f, t, PAD + rows:PAD + all_rows, :] = other[f, :, t * LANES:(t + 1) * LANES]
    for k in range(4):
        copies[k].wait()
    for h in range(2):
        for f in range(5):
            for r in range(0, rows, fold):
                if f < 4:
                    off = 32 * f
                    at_r, at_l = from_r[h, r:r + fold, :], from_l[h, r:r + fold, :]
                else:
                    off = 32 * (r // fold)
                    at_r, at_l = from_r[h, rows:rows + fold, :], from_l[h, rows:rows + fold, :]
                edge = jnp.where(
                    lane_f < HALO, rolled(at_r, -off, 1),
                    jnp.where(lane_f >= LANES - HALO, rolled(at_l, LANES - HALO - off, 1), 0.0),
                )
                start = PAD + h * rows + r
                field[f, own_tiles, start:start + fold, :] = edge

    def wrap(ref, t):
        ref[t, 0:PAD, :] = ref[t, all_rows:all_rows + PAD, :]
        ref[t, PAD + all_rows:2 * PAD + all_rows, :] = ref[t, PAD:2 * PAD, :]

    for f in range(2):
        for t in range(tiles):
            wrap(field.at[f], t)

    chunk = 16
    lane_c = lax.broadcasted_iota(jnp.int32, (chunk, LANES), 1)

    def along(values, offset):
        shifted = [rolled(v, -offset, 1) for v in values]
        step = 1 if offset > 0 else -1
        keep = lane_c < LANES - offset if offset > 0 else lane_c >= -offset
        return [
            jnp.where(keep, shifted[t], shifted[(t + step) % tiles]) for t in range(tiles)
        ]

    offsets = (-2, -1, 1, 2)
    plain = {-2: 1.0 / 12.0, -1: -4.0 / 3.0, 1: -4.0 / 3.0, 2: 1.0 / 12.0}
    speed = {-2: 1.0 / 24.0, -1: -1.0 / 3.0, 1: 1.0 / 3.0, 2: -1.0 / 24.0}

    for r in range(0, all_rows, chunk):
        here = slice(PAD + r, PAD + r + chunk)
        vy = [field[2, t, here, :] for t in range(tiles)]
        for n, o in enumerate(offsets):
            moved = along(vy, o)
            for t in range(tiles):
                vx = field[1, t, here, :]
                vx_o = field[1, t, PAD + r + o:PAD + r + o + chunk, :]
                coef[n, t, r:r + chunk, :] = plain[o] + speed[o] * (vx + vx_o)
                coef[4 + n, t, r:r + chunk, :] = plain[o] + speed[o] * (vy[t] + moved[t])
        for t in range(tiles):
            centre[t, r:r + chunk, :] = 5.0 + field[3, t, here, :]

    def operate(src, r):
        here = slice(PAD + r, PAD + r + chunk)
        u = [src[t, here, :] for t in range(tiles)]
        total = [centre[t, r:r + chunk, :] * u[t] for t in range(tiles)]
        for n, o in enumerate(offsets):
            moved = along(u, o)
            for t in range(tiles):
                u_o = src[t, PAD + r + o:PAD + r + o + chunk, :]
                total[t] = total[t] + (
                    coef[n, t, r:r + chunk, :] * u_o + coef[4 + n, t, r:r + chunk, :] * moved[t]
                )
        return u, total

    x0 = field.at[0]
    for r in range(0, all_rows, chunk):
        here = slice(PAD + r, PAD + r + chunk)
        _, total = operate(x0, r)
        for t in range(tiles):
            r0 = field[4, t, here, :] - total[t]
            vec[1, t, here, :] = r0
            vec[0, t, here, :] = jnp.zeros_like(r0)
            if r < rows and t < own_tiles:
                app[RESTART, t, r:r + chunk, :] = r0
    for t in range(tiles):
        wrap(vec.at[1], t)

    def step(k, carry):
        src = vec.at[k + 1]
        a = jnp.where(k == 0, 1.0 / HALF_WIDTH, 2.0 / HALF_WIDTH).astype(jnp.float32)
        for r in range(0, all_rows, chunk):
            here = slice(PAD + r, PAD + r + chunk)
            u, total = operate(src, r)
            for t in range(tiles):
                if r < rows and t < own_tiles:
                    app[k, t, r:r + chunk, :] = total[t]
                vec[k + 2, t, here, :] = a * (total[t] - CENTRE * u[t]) - vec[k, t, here, :]
        for t in range(tiles):
            wrap(vec.at[k + 2], t)
        return carry

    lax.fori_loop(0, RESTART, step, 0)

    size = RESTART + 1
    places = [(t, r) for t in range(own_tiles) for r in range(0, rows, 8)]
    for i in range(size):
        mine = [app[i, t, r:r + 8, :] for t, r in places]
        for j in range(i + 1):
            if j == i:
                value = tree([m * m for m in mine], lambda a, b: a + b)
            else:
                value = tree(
                    [m * app[j, t, r:r + 8, :] for m, (t, r) in zip(mine, places)],
                    lambda a, b: a + b,
                )
            for p, q in {(i, j), (j, i)}:
                at = (p * size + q) * 8
                acc[at:at + 8, :] = value

    packed = jnp.zeros((8, LANES), jnp.float32)
    for i in range(size):
        for h in range(2):
            base = (i * size + 8 * h) * 8
            pair = tree(
                [
                    (acc[pl.ds(base + s, 8, stride=8), :], jnp.zeros((8, LANES), jnp.float32))
                    for s in range(8)
                ],
                add_pairs,
            )
            shift = LANES // 2
            while shift:
                pair = add_pairs(pair, tuple(rolled(p, shift, 1) for p in pair))
                shift //= 2
            packed = jnp.where(lane == 32 * h + i, pair[0], packed)
            packed = jnp.where(lane == 32 * h + 16 + i, pair[1], packed)
    gram[me, 0:4, :] = jnp.where(
        lane < LANES // 2, packed, rolled(rolled(packed, 4, 0), LANES // 2, 1)
    )[0:4]

    def gram_copy(core, there):
        source = core * ny_dev + there
        return pltpu.make_async_remote_copy(
            src_ref=gram.at[me, 0:4], dst_ref=gram.at[me, 0:4], send_sem=gram_out.at[source],
            recv_sem=gram_in.at[me], device_id=(core, there), device_id_type=MESH,
        )

    def gram_send(step, carry):
        there = lax.rem(gy + step, ny_dev)
        for core in (gx, partner):
            gram_copy(core, there).start()
        return carry

    lax.fori_loop(1, ny_dev, gram_send, 0)
    gram_copy(partner, gy).start()

    def gram_done(core, there):
        source = core * ny_dev + there
        pltpu.make_async_remote_copy(
            src_ref=gram.at[me, 0:4], dst_ref=gram.at[source, 0:4],
            send_sem=gram_out.at[source], recv_sem=gram_in.at[source],
            device_id=(core, there), device_id_type=MESH,
        ).wait()

    def gram_wait(step, carry):
        there = lax.rem(gy + step, ny_dev)
        for core in (gx, partner):
            gram_done(core, there)
        return carry

    gram_done(partner, gy)
    lax.fori_loop(1, ny_dev, gram_wait, 0)

    lane_4 = lax.broadcasted_iota(jnp.int32, (4, LANES), 1)

    def as_pair(value):
        return (
            jnp.where(lane_4 % 32 < 16, value, 0.0),
            jnp.where(lane_4 % 32 < 16, rolled(value, -16, 1), 0.0),
        )

    total = tree([as_pair(gram[d, 0:4, :]) for d in range(n_dev)], add_pairs)

    row_g = lax.broadcasted_iota(jnp.int32, (size, LANES), 0)
    lane_g = lax.broadcasted_iota(jnp.int32, (size, LANES), 1)

    def unpack(value):
        quarters = [rolled(value, -shift, 1) for shift in (0, 64, 32, 96)]
        return jnp.where(lane_g < 16, jnp.concatenate(quarters, axis=0), 0.0)

    g_high, g_low = unpack(total[0]), unpack(total[1])
    m = g_high + jnp.where(lane_g - 16 == row_g, 1.0, 0.0)
    for k in range(RESTART):
        pivot = m[k:k + 1, :] / m[k:k + 1, k:k + 1]
        m = jnp.where(row_g == k, pivot, m - m[:, k:k + 1] * pivot)
    z = jnp.where(row_g < RESTART, jnp.broadcast_to(m[:, RESTART:size], m.shape), -1.0)
    inverse = jnp.where((lane_g < RESTART) & (row_g < RESTART), rolled(m, -16, 1), 0.0)
    for _ in range(REFINEMENTS):
        high, low = two_product(g_high, z)
        low = low + g_low * z
        pair = add_pairs((high[0:8], low[0:8]), (high[8:16], low[8:16]))
        for shift in (4, 2, 1):
            pair = add_pairs(pair, tuple(rolled(p, shift, 0) for p in pair))
        rest = pair[0] + pair[1]
        change = inverse * jnp.concatenate([rest, rest], axis=0)
        z = z - jnp.sum(change, axis=1, keepdims=True)

    weights = [jnp.broadcast_to(z[k:k + 1, :], (8, LANES)) for k in range(RESTART)]
    for t, r in places:
        at = slice(t * LANES, (t + 1) * LANES)
        up = tree(
            [weights[k] * vec[1 + k, t, PAD + r:PAD + r + 8, :] for k in range(RESTART)],
            lambda a, b: a + b,
        )
        sol_ref[r:r + 8, at] = up
        down = tree(
            [weights[k] * app[k, t, r:r + 8, :] for k in range(RESTART)], lambda a, b: a + b
        )
        res_ref[r:r + 8, at] = (b_ref[r:r + 8, at] - app[RESTART, t, r:r + 8, :]) + down


def shards(nx_dev, ny_dev, right_side, initial, reaction, velocity_x, velocity_y):
    rows, cols = right_side.shape
    tiles = cols // LANES + 1
    all_rows = nx_dev * rows
    n_dev = nx_dev * ny_dev
    size = RESTART + 1
    padded = all_rows + 2 * PAD
    pack = (rows + rows // 4, LANES)
    f32 = jnp.float32
    out = jax.ShapeDtypeStruct((rows, cols), f32)
    vmem = pl.BlockSpec(memory_space=pltpu.VMEM)
    update, applied = pl.pallas_call(
        functools.partial(kernel, nx_dev, ny_dev),
        out_shape=(out, out),
        in_specs=[vmem] * 5,
        out_specs=(vmem, vmem),
        scratch_shapes=[
            pltpu.VMEM(pack, f32),
            pltpu.VMEM(pack, f32),
            pltpu.VMEM((2,) + pack, f32),
            pltpu.VMEM((2,) + pack, f32),
            pltpu.VMEM((5, rows, cols), f32),
            pltpu.VMEM((5, tiles, padded, LANES), f32),
            pltpu.VMEM((8, tiles, all_rows, LANES), f32),
            pltpu.VMEM((tiles, all_rows, LANES), f32),
            pltpu.VMEM((RESTART + 2, tiles, padded, LANES), f32),
            pltpu.VMEM((size, cols // LANES, rows, LANES), f32),
            pltpu.VMEM((size * size * 8, LANES), f32),
            pltpu.VMEM((n_dev, 8, LANES), f32),
            pltpu.SemaphoreType.DMA((9,)),
            pltpu.SemaphoreType.DMA((9,)),
            pltpu.SemaphoreType.DMA((n_dev,)),
            pltpu.SemaphoreType.DMA((n_dev,)),
        ],
        compiler_params=pltpu.CompilerParams(collective_id=0, has_side_effects=True),
        name="gmres_cycle",
    )(right_side, initial, reaction, velocity_x, velocity_y)
    return initial + update, right_side - applied


def solution(mesh):
    spec = P("gx", "gy")
    return jax.shard_map(
        functools.partial(shards, mesh.shape["gx"], mesh.shape["gy"]),
        mesh=mesh,
        in_specs=(spec,) * 5,
        out_specs=(spec, spec),
        check_vma=False,
    )
```
